32 devices in a mesh: gx: 8 (over y, x, core), gy: 4 (over z).
Axes of the slice: x: 2, y: 2, z: 4, core: 2. Of those that a mesh axis runs over, the one named last changes fastest.
Arguments:
- populations: float32 [19, 128, 128, 128], P(None, 'gx', 'gy'), may hold values from 0 to 10, as said below
- solid: int32 [128, 128, 128], P('gx', 'gy'), may hold values 0 or 1
Outputs:
- advanced: float32 [19, 128, 128, 128], P(None, 'gx', 'gy')
The draws below stay inside these ranges and needn't reach their ends.
Inputs may be any that keep to these rules, and one draw needn't show every extreme that they name: populations are positive, each between 0.5 w_i 18 and 1.5 w_i 18.
All inputs are finite; a program needn't handle non-finite values. No bound on the sum of `solid` on one device may be relied on, other than what follows from the above.
Results may differ from the reference program's by a relative error of at most 0.0001.
Values sent between devices are 32-bit elements; how exact they have to be, the bound alone decides.
A program may use at most 128 MiB of HBM per device.

```python
import jax
import jax.numpy as jnp
import numpy as np
from jax import lax

NZ = 128
ITERS = 3
NX = 128
NY = 128


def draw_populations(key, part):
    weights = jnp.array([1.0 / 3.0] + [1.0 / 18.0] * 6 + [1.0 / 36.0] * 12, jnp.float32)
    rough = jax.random.uniform(key, (19, NX, NY, NZ), jnp.float32, -1.0, 1.0)
    factor = 1.0 + 0.45 * rough
    return (18.0 * weights[:, None, None, None] * factor).astype(jnp.float32)


def set_ends(entries, key, least, high):
    place = [jax.random.randint(jax.random.fold_in(key, axis), (), 0, length) for axis, length in enumerate(entries.shape)]
    widest = entries.shape.index(max(entries.shape))
    beside = place[:widest] + [(place[widest] + 1) % entries.shape[widest]] + place[widest + 1:]
    return entries.at[tuple(place)].set(least).at[tuple(beside)].set(high)


def setup_inputs(seed: int = 0) -> dict:
    key_of = jax.random.split(jax.random.key(seed), 3)
    populations = draw_populations(jax.random.fold_in(key_of[2], 71), 0)
    solid = set_ends((jax.random.randint(key_of[1], (NX, NY, NZ), 0, 8) < 1).astype(jnp.int32), jax.random.fold_in(key_of[1], 1), 0, 1)
    return {"populations": populations, "solid": solid}


velocity_table = np.array([[0, 0, 0], [1, 0, 0], [-1, 0, 0], [0, 1, 0], [0, -1, 0], [0, 0, 1], [0, 0, -1], [1, 1, 0], [-1, -1, 0], [1, -1, 0], [-1, 1, 0], [1, 0, 1], [-1, 0, -1], [1, 0, -1], [-1, 0, 1], [0, 1, 1], [0, -1, -1], [0, 1, -1], [0, -1, 1]])
weight_table = np.array([1.0 / 3.0] + [1.0 / 18.0] * 6 + [1.0 / 36.0] * 12)
relax = 1.6


def opposite(index):
    if index == 0:
        return 0
    return index + 1 if index % 2 == 1 else index - 1


def collide(field, fluid):
    table = jnp.asarray(velocity_table, jnp.float32)
    weights = jnp.asarray(weight_table, jnp.float32)
    density = jnp.sum(field, axis=0)
    moment = jnp.tensordot(table.T, field, axes=1, precision=lax.Precision.HIGHEST)
    speed = moment / density
    along = jnp.tensordot(table, speed, axes=1, precision=lax.Precision.HIGHEST)
    square = jnp.sum(speed * speed, axis=0)
    balance = weights[:, None, None, None] * density * (1.0 + 3.0 * along + 4.5 * along * along - 1.5 * square)
    return jnp.where(fluid, field + relax * (balance - field), field)


def reference(populations, solid):
    fluid = solid == 0
    field = populations
    for step in range(ITERS):
        post = collide(field, fluid)
        result = []
        for index in range(19):
            shift = tuple(int(v) for v in velocity_table[index])
            source = jnp.roll(post[index], shift, axis=(0, 1, 2))
            blocked = jnp.roll(solid, shift, axis=(0, 1, 2)) != 0
            value = jnp.where(blocked, post[opposite(index)], source)
            result.append(jnp.where(fluid, value, post[index]))
        field = jnp.stack(result)
    return field
```

```python
import functools

import jax
import jax.numpy as jnp
from jax import lax
from jax.experimental import pallas as pl
from jax.experimental.pallas import tpu as pltpu
from jax.sharding import PartitionSpec as P

ITERS = 3
MESH = pl.DeviceIdType.MESH

VELOCITY = (
    (0, 0, 0),
    (1, 0, 0), (-1, 0, 0), (0, 1, 0), (0, -1, 0), (0, 0, 1), (0, 0, -1),
    (1, 1, 0), (-1, -1, 0), (1, -1, 0), (-1, 1, 0),
    (1, 0, 1), (-1, 0, -1), (1, 0, -1), (-1, 0, 1),
    (0, 1, 1), (0, -1, -1), (0, 1, -1), (0, -1, 1),
)
RELAX = 1.6
BIG = 1e37
BLOCKED = 1e34

ORDER = [9, 1, 11, 13, 7, 3, 15, 17, 10, 2, 12, 14, 8, 4, 16, 18, 0, 5, 6]
SLOT = {index: slot for slot, index in enumerate(ORDER)}
UP_Y = [7, 3, 15, 17, 10]
DOWN_Y = [8, 4, 16, 18, 9]
CORNERS = (7, 8, 9, 10)
PAD = 8


def opposite(index):
    if index == 0:
        return 0
    return index + 1 if index % 2 == 1 else index - 1


def collide(f, fluid, wanted=range(19)):
    total = {}
    delta = {}
    for i in range(1, 19, 2):
        total[i] = f[i] + f[i + 1]
        delta[i] = f[i] - f[i + 1]
    rho = f[0] + ((total[1] + total[3]) + (total[5] + total[7])) + (
        ((total[9] + total[11]) + (total[13] + total[15])) + total[17]
    )
    mx = (delta[1] + delta[7]) + (delta[9] + delta[11]) + delta[13]
    my = (delta[3] + delta[7]) + (delta[15] - delta[9]) + delta[17]
    mz = (delta[5] + delta[11]) + (delta[15] - delta[13]) - delta[17]
    zero = jnp.zeros_like(rho)
    scale = RELAX * 3.0 / 36.0
    mx = jnp.where(fluid, mx * scale, zero)
    my = jnp.where(fluid, my * scale, zero)
    mz = jnp.where(fluid, mz * scale, zero)
    inv = 1.0 / rho
    curve = inv * (RELAX * 4.5 / 36.0 / (scale * scale))
    base = rho * (RELAX / 36.0) - (mx * mx + my * my + mz * mz) * (
        inv * (RELAX * 1.5 / 36.0 / (scale * scale))
    )
    base = jnp.where(fluid, base, jnp.full_like(rho, BIG * RELAX / 36.0))
    post = [None] * 19
    keep = 1.0 - RELAX
    half = keep * 0.5
    if 0 in wanted:
        post[0] = base * 12.0 + f[0] * keep
    base2 = base + base
    curve2 = curve + curve
    for i in range(1, 19, 2):
        if i not in wanted and i + 1 not in wanted:
            continue
        cx, cy, cz = VELOCITY[i]
        along = None
        for c, m in ((cx, mx), (cy, my), (cz, mz)):
            if c == 0:
                continue
            if along is None:
                along = m
            else:
                along = along + m if c > 0 else along - m
        if i < 7:
            even = base2 + along * along * curve2
            odd = along + along
        else:
            even = base + along * along * curve
            odd = along
        even = even + total[i] * half
        odd = odd + delta[i] * half
        if i in wanted:
            post[i] = even + odd
        if i + 1 in wanted:
            post[i + 1] = even - odd
    return post


def pull(load):
    own = [load(SLOT[i], 0, 0) for i in range(19)]
    f = [own[0]]
    for i in range(1, 19):
        cx, cy, cz = VELOCITY[i]
        value = own[i] if cx == 0 and cy == 0 else load(SLOT[i], cx, cy)
        if cz:
            value = pltpu.roll(value, 1 if cz > 0 else value.shape[1] - 1, axis=1)
        f.append(jnp.where(value > BLOCKED, own[opposite(i)], value))
    return f


def flatten(buf):
    count, planes, pitch, lanes = buf.shape
    return buf.reshape(count, planes * pitch, lanes)


def tile_load(buf, x, t):
    pitch = buf.shape[2]
    view = flatten(buf)

    def load(slot, cx, cy):
        first = PAD + 8 * t - cy
        if first + 8 > pitch:
            return view[slot, pl.ds((x + 1 - cx) * pitch + first, 8), :]
        return buf[slot, x + 1 - cx, pl.ds(first, 8), :]

    return load


def step_kernel(sizes, axes, f_hbm, solid_hbm, p2, field, solid, p0, p1, f_row, s_row, y_send, in_sem, send_sem, recv_sem):
    rows, cols, gx_size, gy_size = sizes
    gx, gy = axes
    tiles = cols // 8
    pitch = cols + PAD
    buffers = (p0, p1, p2)
    flat = [flatten(buf) for buf in buffers]
    me_x, me_y = lax.axis_index(gx), lax.axis_index(gy)
    up_x, down_x = lax.rem(me_x + 1, gx_size), lax.rem(me_x + gx_size - 1, gx_size)
    up_y, down_y = lax.rem(me_y + 1, gy_size), lax.rem(me_y + gy_size - 1, gy_size)
    place_x = {1: up_x, 0: me_x, -1: down_x}
    place_y = {1: up_y, 0: me_y, -1: down_y}

    def device(dx, dy):
        return {gx: place_x[dx], gy: place_y[dy]}

    pairs = (rows - 2) // 2
    edge_y = (cols - 1, 0)

    def load(start, count, sem):
        return pltpu.make_async_copy(
            f_hbm.at[:, pl.ds(start, count)], field.at[:, pl.ds(start, count)], in_sem.at[sem]
        )

    barrier = pltpu.get_barrier_semaphore()
    around = [(dx, dy) for dx in (-1, 0, 1) for dy in (-1, 0, 1) if (dx, dy) != (0, 0)]
    for dx, dy in around:
        pl.semaphore_signal(barrier, inc=1, device_id=device(dx, dy), device_id_type=MESH)

    row_loads = []
    for side, y in enumerate(edge_y):
        row_loads.append(pltpu.make_async_copy(f_hbm.at[:, :, y], f_row.at[side], in_sem.at[2 * side]))
        row_loads.append(pltpu.make_async_copy(solid_hbm.at[:, y], s_row.at[side], in_sem.at[2 * side + 1]))
    for copy in row_loads:
        copy.start()
    load_solid = pltpu.make_async_copy(solid_hbm, solid, in_sem.at[4])
    load_solid.start()
    ends = [load(0, 1, 5), load(rows - 1, 1, 6)]
    inner = [load(1 + 2 * c, 2, 7 + c) for c in range(pairs)]
    for copy in ends + inner:
        copy.start()

    def remote(src, dst, phase, which, dx, dy):
        return pltpu.make_async_remote_copy(
            src_ref=src,
            dst_ref=dst,
            send_sem=send_sem.at[phase, which],
            recv_sem=recv_sem.at[phase, which],
            device_id=device(dx, dy),
            device_id_type=MESH,
        )

    def x_copies(phase):
        buf = buffers[phase]
        own = pl.ds(PAD, cols)
        up, down = pl.ds(0, 5), pl.ds(8, 5)
        return [
            remote(buf.at[up, rows, own], buf.at[up, 0, own], phase, 0, 1, 0),
            remote(buf.at[down, 1, own], buf.at[down, rows + 1, own], phase, 1, -1, 0),
        ]

    def corner_copies(phase):
        buf = buffers[phase]
        copies = []
        for k, index in enumerate(CORNERS):
            cx, cy, _ = VELOCITY[index]
            side = 0 if cy > 0 else 1
            j = (UP_Y, DOWN_Y)[side].index(index)
            src_x, dst_x = (rows - 1, 0) if cx > 0 else (0, rows + 1)
            dst = buf.at[SLOT[index], dst_x, PAD - 1] if cy > 0 else buf.at[SLOT[index], dst_x + 1, 0]
            copies.append(remote(y_send.at[phase, side, j, src_x], dst, phase, 2 + k, cx, cy))
        return copies

    def y_copies(phase):
        buf = buffers[phase]
        return [
            remote(y_send.at[phase, 0], buf.at[pl.ds(4, 5), pl.ds(1, rows), PAD - 1], phase, 6, 0, 1),
            remote(y_send.at[phase, 1, pl.ds(0, 4)], buf.at[pl.ds(12, 4), pl.ds(2, rows), 0], phase, 7, 0, -1),
            remote(y_send.at[phase, 1, 4], buf.at[0, pl.ds(2, rows), 0], phase, 8, 0, -1),
        ]

    def row(phase, side, g):
        fluid = s_row[side, pl.ds(8 * g, 8), :] == 0
        if phase == 0:
            f = [f_row[side, i, pl.ds(8 * g, 8), :] for i in range(19)]
        else:
            view = flat[phase - 1]

            def strided(slot, cx, cy):
                start = (8 * g + 1 - cx) * pitch + PAD + edge_y[side] - cy
                return view[slot, pl.ds(start, 8, stride=pitch), :]

            f = pull(strided)
        wanted = (UP_Y, DOWN_Y)[side]
        post = collide(f, fluid, wanted)
        for j, index in enumerate(wanted):
            y_send[phase, side, j, pl.ds(8 * g, 8), :] = post[index]

    def advance(phase, x, t):
        fluid = solid[x, pl.ds(8 * t, 8), :] == 0
        if phase == 0:
            f = [field[i, x, pl.ds(8 * t, 8), :] for i in range(19)]
        else:
            f = pull(tile_load(buffers[phase - 1], x, t))
        post = collide(f, fluid)
        for i in range(19):
            buffers[phase][SLOT[i], x + 1, pl.ds(PAD + 8 * t, 8), :] = post[i]

    def plane(phase, x):
        for t in range(tiles):
            advance(phase, x, t)

    def start(copies):
        for copy in copies:
            copy.start()

    for phase in range(ITERS):
        if phase == 0:
            for copy in row_loads:
                copy.wait()
        else:
            for copy in x_copies(phase - 1) + y_copies(phase - 1) + corner_copies(phase - 1):
                copy.wait_recv()
        for side in range(2):
            for g in range(rows // 8):
                row(phase, side, g)
        if phase == 0:
            pl.semaphore_wait(barrier, len(around))
        start(corner_copies(phase))
        start(y_copies(phase))
        if phase == 0:
            load_solid.wait()
            for copy in ends:
                copy.wait()
        plane(phase, rows - 1)
        plane(phase, 0)
        start(x_copies(phase))
        if phase == 0:
            for copy in inner:
                copy.wait()

        def step(x, carry):
            plane(phase, x)
            return carry

        lax.fori_loop(1, rows - 1, step, 0)

    last = ITERS - 1
    for copy in x_copies(last) + y_copies(last) + corner_copies(last):
        copy.wait_recv()
    for phase in range(ITERS):
        for copy in x_copies(phase) + y_copies(phase) + corner_copies(phase):
            copy.wait_send()


def finish_kernel(buf, field, out, stage, sem):
    count, rows, cols, _ = stage.shape

    def copy(x):
        return pltpu.make_async_copy(stage.at[:, x], out.at[:, x], sem.at[x])

    def step(x, carry):
        for t in range(cols // 8):
            load = tile_load(buf, x, t)
            f = pull(load)
            fluid = f[0] < BLOCKED
            for i in range(count):
                kept = field[i, x, pl.ds(8 * t, 8), :]
                stage[i, x, pl.ds(8 * t, 8), :] = jnp.where(fluid, f[i], kept)
        copy(x).start()
        return carry

    lax.fori_loop(0, rows, step, 0)
    for x in range(rows):
        copy(x).wait()


def solution(mesh):
    gx, gy = mesh.axis_names
    gx_size, gy_size = mesh.shape[gx], mesh.shape[gy]

    def local(populations, solid):
        count, rows, cols, lanes = populations.shape
        f32 = jnp.float32
        padded = (count, rows + 3, cols + PAD, lanes)
        vmem = pl.BlockSpec(memory_space=pltpu.VMEM)
        hbm = pl.BlockSpec(memory_space=pltpu.HBM)
        post, field = pl.pallas_call(
            functools.partial(step_kernel, (rows, cols, gx_size, gy_size), (gx, gy)),
            out_shape=(
                jax.ShapeDtypeStruct(padded, f32),
                jax.ShapeDtypeStruct(populations.shape, f32),
            ),
            in_specs=[hbm, hbm],
            out_specs=(vmem, vmem),
            scratch_shapes=[
                pltpu.VMEM((rows, cols, lanes), jnp.int32),
                pltpu.VMEM(padded, f32),
                pltpu.VMEM(padded, f32),
                pltpu.VMEM((2, count, rows, lanes), f32),
                pltpu.VMEM((2, rows, lanes), jnp.int32),
                pltpu.VMEM((ITERS, 2, 5, rows, lanes), f32),
                pltpu.SemaphoreType.DMA((7 + (rows - 2) // 2,)),
                pltpu.SemaphoreType.DMA((ITERS, 9)),
                pltpu.SemaphoreType.DMA((ITERS, 9)),
            ],
            compiler_params=pltpu.CompilerParams(
                collective_id=0, has_side_effects=True, vmem_limit_bytes=30 * 1024 * 1024
            ),
        )(
            pltpu.with_memory_space_constraint(populations, pltpu.HBM),
            pltpu.with_memory_space_constraint(solid, pltpu.HBM),
        )
        return pl.pallas_call(
            finish_kernel,
            out_shape=jax.ShapeDtypeStruct(populations.shape, f32),
            in_specs=[vmem, vmem],
            out_specs=hbm,
            scratch_shapes=[
                pltpu.VMEM(populations.shape, f32),
                pltpu.SemaphoreType.DMA((rows,)),
            ],
            compiler_params=pltpu.CompilerParams(vmem_limit_bytes=12 * 1024 * 1024),
        )(post, field)

    return jax.shard_map(
        local,
        mesh=mesh,
        in_specs=(P(None, gx, gy, None), P(gx, gy, None)),
        out_specs=P(None, gx, gy, None),
        check_vma=False,
    )
```

```python
import functools

import jax
import jax.numpy as jnp
from jax import lax
from jax.experimental import pallas as pl
from jax.experimental.pallas import tpu as pltpu
from jax.sharding import PartitionSpec as P

ITERS = 3
MESH = pl.DeviceIdType.MESH

VELOCITY = (
    (0, 0, 0),
    (1, 0, 0), (-1, 0, 0), (0, 1, 0), (0, -1, 0), (0, 0, 1), (0, 0, -1),
    (1, 1, 0), (-1, -1, 0), (1, -1, 0), (-1, 1, 0),
    (1, 0, 1), (-1, 0, -1), (1, 0, -1), (-1, 0, 1),
    (0, 1, 1), (0, -1, -1), (0, 1, -1), (0, -1, 1),
)
RELAX = 1.6
BIG = 1e37
BLOCKED = 1e34

ORDER = [9, 1, 11, 13, 7, 3, 15, 17, 10, 2, 12, 14, 8, 4, 16, 18, 0, 5, 6]
SLOT = {index: slot for slot, index in enumerate(ORDER)}
UP_Y = [7, 3, 15, 17, 10]
DOWN_Y = [8, 4, 16, 18, 9]
CORNERS = (7, 8, 9, 10)
PAD = 8


def opposite(index):
    if index == 0:
        return 0
    return index + 1 if index % 2 == 1 else index - 1


def collide(f, fluid, wanted=range(19)):
    total = {}
    delta = {}
    for i in range(1, 19, 2):
        total[i] = f[i] + f[i + 1]
        delta[i] = f[i] - f[i + 1]
    rho = f[0] + ((total[1] + total[3]) + (total[5] + total[7])) + (
        ((total[9] + total[11]) + (total[13] + total[15])) + total[17]
    )
    mx = (delta[1] + delta[7]) + (delta[9] + delta[11]) + delta[13]
    my = (delta[3] + delta[7]) + (delta[15] - delta[9]) + delta[17]
    mz = (delta[5] + delta[11]) + (delta[15] - delta[13]) - delta[17]
    zero = jnp.zeros_like(rho)
    scale = RELAX * 3.0 / 36.0
    mx = jnp.where(fluid, mx * scale, zero)
    my = jnp.where(fluid, my * scale, zero)
    mz = jnp.where(fluid, mz * scale, zero)
    inv = 1.0 / rho
    curve = inv * (RELAX * 4.5 / 36.0 / (scale * scale))
    base = rho * (RELAX / 36.0) - (mx * mx + my * my + mz * mz) * (
        inv * (RELAX * 1.5 / 36.0 / (scale * scale))
    )
    base = jnp.where(fluid, base, jnp.full_like(rho, BIG * RELAX / 36.0))
    post = [None] * 19
    keep = 1.0 - RELAX
    half = keep * 0.5
    if 0 in wanted:
        post[0] = base * 12.0 + f[0] * keep
    base2 = base + base
    curve2 = curve + curve
    for i in range(1, 19, 2):
        if i not in wanted and i + 1 not in wanted:
            continue
        cx, cy, cz = VELOCITY[i]
        along = None
        for c, m in ((cx, mx), (cy, my), (cz, mz)):
            if c == 0:
                continue
            if along is None:
                along = m
            else:
                along = along + m if c > 0 else along - m
        if i < 7:
            even = base2 + along * along * curve2
            odd = along + along
        else:
            even = base + along * along * curve
            odd = along
        even = even + total[i] * half
        odd = odd + delta[i] * half
        if i in wanted:
            post[i] = even + odd
        if i + 1 in wanted:
            post[i + 1] = even - odd
    return post


def pull(load):
    own = [load(SLOT[i], 0, 0) for i in range(19)]
    f = [own[0]]
    for i in range(1, 19):
        cx, cy, cz = VELOCITY[i]
        value = own[i] if cx == 0 and cy == 0 else load(SLOT[i], cx, cy)
        if cz:
            value = pltpu.roll(value, 1 if cz > 0 else value.shape[1] - 1, axis=1)
        f.append(jnp.where(value > BLOCKED, own[opposite(i)], value))
    return f


def flatten(buf):
    count, planes, pitch, lanes = buf.shape
    return buf.reshape(count, planes * pitch, lanes)


def tile_load(buf, x, t):
    pitch = buf.shape[2]
    view = flatten(buf)

    def load(slot, cx, cy):
        first = PAD + 8 * t - cy
        if first + 8 > pitch:
            return view[slot, pl.ds((x + 1 - cx) * pitch + first, 8), :]
        return buf[slot, x + 1 - cx, pl.ds(first, 8), :]

    return load


def step_kernel(sizes, axes, f_hbm, solid_hbm, p2, field, solid, p0, p1, f_row, s_row, y_send, in_sem, send_sem, recv_sem):
    rows, cols, gx_size, gy_size = sizes
    gx, gy = axes
    tiles = cols // 8
    pitch = cols + PAD
    sent = 10 * (rows + cols) + len(CORNERS)
    buffers = (p0, p1, p2)
    flat = [flatten(buf) for buf in buffers]
    me_x, me_y = lax.axis_index(gx), lax.axis_index(gy)
    up_x, down_x = lax.rem(me_x + 1, gx_size), lax.rem(me_x + gx_size - 1, gx_size)
    up_y, down_y = lax.rem(me_y + 1, gy_size), lax.rem(me_y + gy_size - 1, gy_size)
    place_x = {1: up_x, 0: me_x, -1: down_x}
    place_y = {1: up_y, 0: me_y, -1: down_y}

    def device(dx, dy):
        return {gx: place_x[dx], gy: place_y[dy]}

    pairs = (rows - 2) // 2
    edge_y = (cols - 1, 0)

    def load(start, count, sem):
        planes = pl.ds(start, count)
        return pltpu.make_async_copy(
            f_hbm.at[:, planes], field.at[:, planes, pl.ds(0, cols)], in_sem.at[sem]
        )

    barrier = pltpu.get_barrier_semaphore()
    around = [(dx, dy) for dx in (-1, 0, 1) for dy in (-1, 0, 1) if (dx, dy) != (0, 0)]
    for dx, dy in around:
        pl.semaphore_signal(barrier, inc=1, device_id=device(dx, dy), device_id_type=MESH)

    row_loads = []
    for side, y in enumerate(edge_y):
        row_loads.append(pltpu.make_async_copy(f_hbm.at[:, :, y], f_row.at[side], in_sem.at[0]))
        row_loads.append(pltpu.make_async_copy(solid_hbm.at[:, y], s_row.at[side], in_sem.at[1 + side]))
    load_solid = pltpu.make_async_copy(solid_hbm, solid, in_sem.at[3])
    ends = [load(0, 1, 4), load(rows - 1, 1, 4)]
    inner = [load(1 + 2 * c, 2, 5) for c in range(pairs)]
    for copy in row_loads + [load_solid] + ends + inner:
        copy.start()

    def wait_rows():
        both = (slice(None), pl.ds(0, 2), pl.ds(0, rows))
        pltpu.make_async_copy(f_hbm.at[both], field.at[both], in_sem.at[0]).wait()
        row_loads[1].wait()
        row_loads[3].wait()

    def remote(src, dst, phase, dx, dy):
        return pltpu.make_async_remote_copy(
            src_ref=src,
            dst_ref=dst,
            send_sem=send_sem.at[0],
            recv_sem=recv_sem.at[phase],
            device_id=device(dx, dy),
            device_id_type=MESH,
        )

    def x_copies(phase):
        buf = buffers[phase]
        own = pl.ds(PAD, cols)
        up, down = pl.ds(0, 5), pl.ds(8, 5)
        return [
            remote(buf.at[up, rows, own], buf.at[up, 0, own], phase, 1, 0),
            remote(buf.at[down, 1, own], buf.at[down, rows + 1, own], phase, -1, 0),
        ]

    def corner_copies(phase):
        buf = buffers[phase]
        copies = []
        for index in CORNERS:
            cx, cy, _ = VELOCITY[index]
            side = 0 if cy > 0 else 1
            j = (UP_Y, DOWN_Y)[side].index(index)
            src_x, dst_x = (rows - 1, 0) if cx > 0 else (0, rows + 1)
            dst = buf.at[SLOT[index], dst_x, PAD - 1] if cy > 0 else buf.at[SLOT[index], dst_x + 1, 0]
            copies.append(remote(y_send.at[phase, side, j, src_x], dst, phase, cx, cy))
        return copies

    def y_copies(phase):
        buf = buffers[phase]
        return [
            remote(y_send.at[phase, 0], buf.at[pl.ds(4, 5), pl.ds(1, rows), PAD - 1], phase, 0, 1),
            remote(y_send.at[phase, 1, pl.ds(0, 4)], buf.at[pl.ds(12, 4), pl.ds(2, rows), 0], phase, 0, -1),
            remote(y_send.at[phase, 1, 4], buf.at[0, pl.ds(2, rows), 0], phase, 0, -1),
        ]

    def arrive(phase):
        view = flat[phase].at[0, pl.ds(0, sent)]
        remote(view, view, phase, 1, 0).wait_recv()

    def row(phase, side, g):
        fluid = s_row[side, pl.ds(8 * g, 8), :] == 0
        if phase == 0:
            f = [f_row[side, i, pl.ds(8 * g, 8), :] for i in range(19)]
        else:
            view = flat[phase - 1]

            def strided(slot, cx, cy):
                start = (8 * g + 1 - cx) * pitch + PAD + edge_y[side] - cy
                return view[slot, pl.ds(start, 8, stride=pitch), :]

            f = pull(strided)
        wanted = (UP_Y, DOWN_Y)[side]
        post = collide(f, fluid, wanted)
        for j, index in enumerate(wanted):
            y_send[phase, side, j, pl.ds(8 * g, 8), :] = post[index]

    def advance(phase, x, t):
        fluid = solid[x, pl.ds(8 * t, 8), :] == 0
        if phase == 0:
            f = [field[i, x, pl.ds(8 * t, 8), :] for i in range(19)]
        else:
            f = pull(tile_load(buffers[phase - 1], x, t))
        post = collide(f, fluid)
        for i in range(19):
            buffers[phase][SLOT[i], x + 1, pl.ds(PAD + 8 * t, 8), :] = post[i]

    def plane(phase, x):
        for t in range(tiles):
            advance(phase, x, t)

    def start(copies):
        for copy in copies:
            copy.start()

    def edge_rows(phase):
        for side in range(2):
            for g in range(rows // 8):
                row(phase, side, g)

    def finish(x, t):
        f = pull(tile_load(p2, x, t))
        fluid = f[0] < BLOCKED
        for i in range(19):
            kept = field[i, x, pl.ds(8 * t, 8), :]
            field[i, x, pl.ds(8 * t, 8), :] = jnp.where(fluid, f[i], kept)

    odd = lax.rem(me_x, 2) == 1

    for phase in range(ITERS):
        if phase == 0:
            wait_rows()
        else:
            arrive(phase - 1)
        edge_rows(phase)
        x_up, x_down = x_copies(phase)
        if phase == 0:
            load_solid.wait()
            load(0, 2, 4).wait()
            plane(phase, rows - 1)
            plane(phase, 0)
            pl.semaphore_wait(barrier, len(around))
        start(corner_copies(phase))

        @pl.when(odd)
        def _():
            if phase:
                plane(phase, rows - 1)
            x_up.start()
            start(y_copies(phase))
            if phase:
                plane(phase, 0)
            x_down.start()

        @pl.when(jnp.logical_not(odd))
        def _():
            start(y_copies(phase))
            if phase:
                plane(phase, 0)
            x_down.start()
            if phase:
                plane(phase, rows - 1)
            x_up.start()

        if phase == 0:
            load(1, rows - 2, 5).wait()

        def step(x, carry):
            plane(phase, x)
            return carry

        lax.fori_loop(1, rows - 1, step, 0)

    def finish_step(c, carry):
        for dx in range(2):
            for t in range(1, tiles - 1):
                finish(1 + 2 * c + dx, t)
        return carry

    lax.fori_loop(0, pairs, finish_step, 0)

    view = flat[0].at[pl.ds(0, ITERS), pl.ds(0, sent)]
    remote(view, view, 0, 1, 0).wait_send()
    arrive(ITERS - 1)


def finish_kernel(buf, field, out, stage, sem):
    count, rows, cols, _ = out.shape
    tiles = cols // 8
    pairs = rows // 2
    inside = pl.ds(8, cols - 16)
    edges = (0, tiles - 1)

    def inner_copy(c):
        where = (slice(None), pl.ds(1 + 2 * c, 2), inside)
        return pltpu.make_async_copy(field.at[where], out.at[where], sem.at[0])

    def edge_copy(c, k):
        where = (slice(None), pl.ds(2 * c, 2), pl.ds(8 * edges[k], 8))
        return pltpu.make_async_copy(stage.at[where], out.at[where], sem.at[0])

    def end_copy(x, k):
        where = (slice(None), x, inside)
        return pltpu.make_async_copy(stage.at[where], out.at[where], sem.at[0])

    def finish(x, t):
        f = pull(tile_load(buf, x, t))
        fluid = f[0] < BLOCKED
        for i in range(count):
            kept = field[i, x, pl.ds(8 * t, 8), :]
            stage[i, x, pl.ds(8 * t, 8), :] = jnp.where(fluid, f[i], kept)

    for c in range(pairs - 1):
        inner_copy(c).start()
    for k, x in enumerate((0, rows - 1)):
        for t in range(1, tiles - 1):
            finish(x, t)
        end_copy(x, k).start()

    def step(c, carry):
        for dx in range(2):
            for t in edges:
                finish(2 * c + dx, t)
        for k in range(2):
            edge_copy(c, k).start()
        return carry

    lax.fori_loop(0, pairs, step, 0)
    pltpu.make_async_copy(stage.at[:, pl.ds(0, rows), pl.ds(0, cols)], out, sem.at[0]).wait()


def solution(mesh):
    gx, gy = mesh.axis_names
    gx_size, gy_size = mesh.shape[gx], mesh.shape[gy]

    def local(populations, solid):
        count, rows, cols, lanes = populations.shape
        f32 = jnp.float32
        padded = (count, rows + 3, cols + PAD, lanes)
        spaced = (count, rows + 1, cols + PAD, lanes)
        vmem = pl.BlockSpec(memory_space=pltpu.VMEM)
        hbm = pl.BlockSpec(memory_space=pltpu.HBM)
        post, field = pl.pallas_call(
            functools.partial(step_kernel, (rows, cols, gx_size, gy_size), (gx, gy)),
            out_shape=(
                jax.ShapeDtypeStruct(padded, f32),
                jax.ShapeDtypeStruct(spaced, f32),
            ),
            in_specs=[hbm, hbm],
            out_specs=(vmem, vmem),
            scratch_shapes=[
                pltpu.VMEM((rows, cols, lanes), jnp.int32),
                pltpu.VMEM(padded, f32),
                pltpu.VMEM(padded, f32),
                pltpu.VMEM((2, count, rows, lanes), f32),
                pltpu.VMEM((2, rows, lanes), jnp.int32),
                pltpu.VMEM((ITERS, 2, 5, rows, lanes), f32),
                pltpu.SemaphoreType.DMA((6,)),
                pltpu.SemaphoreType.DMA((1,)),
                pltpu.SemaphoreType.DMA((ITERS,)),
            ],
            compiler_params=pltpu.CompilerParams(
                collective_id=0, has_side_effects=True, vmem_limit_bytes=30 * 1024 * 1024
            ),
        )(
            pltpu.with_memory_space_constraint(populations, pltpu.HBM),
            pltpu.with_memory_space_constraint(solid, pltpu.HBM),
        )
        return pl.pallas_call(
            finish_kernel,
            out_shape=jax.ShapeDtypeStruct(populations.shape, f32),
            in_specs=[vmem, vmem],
            out_specs=hbm,
            scratch_shapes=[
                pltpu.VMEM(spaced, f32),
                pltpu.SemaphoreType.DMA((1,)),
            ],
            compiler_params=pltpu.CompilerParams(vmem_limit_bytes=12 * 1024 * 1024),
        )(post, field)

    return jax.shard_map(
        local,
        mesh=mesh,
        in_specs=(P(None, gx, gy, None), P(gx, gy, None)),
        out_specs=P(None, gx, gy, None),
        check_vma=False,
    )
```

```python
import functools

import jax
import jax.numpy as jnp
from jax import lax
from jax.experimental import pallas as pl
from jax.experimental.pallas import tpu as pltpu
from jax.sharding import PartitionSpec as P

ITERS = 3
MESH = pl.DeviceIdType.MESH

VELOCITY = (
    (0, 0, 0),
    (1, 0, 0), (-1, 0, 0), (0, 1, 0), (0, -1, 0), (0, 0, 1), (0, 0, -1),
    (1, 1, 0), (-1, -1, 0), (1, -1, 0), (-1, 1, 0),
    (1, 0, 1), (-1, 0, -1), (1, 0, -1), (-1, 0, 1),
    (0, 1, 1), (0, -1, -1), (0, 1, -1), (0, -1, 1),
)
RELAX = 1.6
BIG = 1e37
BLOCKED = 1e34

ORDER = [9, 1, 11, 13, 7, 3, 15, 17, 10, 2, 12, 14, 8, 4, 16, 18, 0, 5, 6]
SLOT = {index: slot for slot, index in enumerate(ORDER)}
UP_Y = [7, 3, 15, 17, 10]
DOWN_Y = [8, 4, 16, 18, 9]
CORNERS = (7, 8, 9, 10)
PAD = 8


def opposite(index):
    if index == 0:
        return 0
    return index + 1 if index % 2 == 1 else index - 1


def collide(f, fluid, wanted=range(19)):
    total = {}
    delta = {}
    for i in range(1, 19, 2):
        total[i] = f[i] + f[i + 1]
        delta[i] = f[i] - f[i + 1]
    rho = f[0] + ((total[1] + total[3]) + (total[5] + total[7])) + (
        ((total[9] + total[11]) + (total[13] + total[15])) + total[17]
    )
    mx = (delta[1] + delta[7]) + (delta[9] + delta[11]) + delta[13]
    my = (delta[3] + delta[7]) + (delta[15] - delta[9]) + delta[17]
    mz = (delta[5] + delta[11]) + (delta[15] - delta[13]) - delta[17]
    zero = jnp.zeros_like(rho)
    scale = RELAX * 3.0 / 36.0
    mx = jnp.where(fluid, mx * scale, zero)
    my = jnp.where(fluid, my * scale, zero)
    mz = jnp.where(fluid, mz * scale, zero)
    inv = 1.0 / rho
    curve = inv * (RELAX * 4.5 / 36.0 / (scale * scale))
    base = rho * (RELAX / 36.0) - (mx * mx + my * my + mz * mz) * (
        inv * (RELAX * 1.5 / 36.0 / (scale * scale))
    )
    base = jnp.where(fluid, base, jnp.full_like(rho, BIG * RELAX / 36.0))
    post = [None] * 19
    keep = 1.0 - RELAX
    half = keep * 0.5
    if 0 in wanted:
        post[0] = base * 12.0 + f[0] * keep
    base2 = base + base
    curve2 = curve + curve
    for i in range(1, 19, 2):
        if i not in wanted and i + 1 not in wanted:
            continue
        cx, cy, cz = VELOCITY[i]
        along = None
        for c, m in ((cx, mx), (cy, my), (cz, mz)):
            if c == 0:
                continue
            if along is None:
                along = m
            else:
                along = along + m if c > 0 else along - m
        if i < 7:
            even = base2 + along * along * curve2
            odd = along + along
        else:
            even = base + along * along * curve
            odd = along
        even = even + total[i] * half
        odd = odd + delta[i] * half
        if i in wanted:
            post[i] = even + odd
        if i + 1 in wanted:
            post[i + 1] = even - odd
    return post


def pull(load):
    own = [load(SLOT[i], 0, 0) for i in range(19)]
    f = [own[0]]
    for i in range(1, 19):
        cx, cy, cz = VELOCITY[i]
        value = own[i] if cx == 0 and cy == 0 else load(SLOT[i], cx, cy)
        if cz:
            value = pltpu.roll(value, 1 if cz > 0 else value.shape[1] - 1, axis=1)
        f.append(jnp.where(value > BLOCKED, own[opposite(i)], value))
    return f


def flatten(buf):
    count, planes, pitch, lanes = buf.shape
    return buf.reshape(count, planes * pitch, lanes)


def tile_load(buf, x, t):
    pitch = buf.shape[2]
    view = flatten(buf)

    def load(slot, cx, cy):
        first = PAD + 8 * t - cy
        if first + 8 > pitch:
            return view[slot, pl.ds((x + 1 - cx) * pitch + first, 8), :]
        return buf[slot, x + 1 - cx, pl.ds(first, 8), :]

    return load


def step_kernel(sizes, axes, f_hbm, solid_hbm, p2, field, solid, p0, p1, f_row, s_row, y_send, in_sem, send_sem, recv_sem):
    rows, cols, gx_size, gy_size = sizes
    gx, gy = axes
    tiles = cols // 8
    pitch = cols + PAD
    sent = 10 * (rows + cols) + len(CORNERS)
    buffers = (p0, p1, p2)
    flat = [flatten(buf) for buf in buffers]
    me_x, me_y = lax.axis_index(gx), lax.axis_index(gy)
    up_x, down_x = lax.rem(me_x + 1, gx_size), lax.rem(me_x + gx_size - 1, gx_size)
    up_y, down_y = lax.rem(me_y + 1, gy_size), lax.rem(me_y + gy_size - 1, gy_size)
    place_x = {1: up_x, 0: me_x, -1: down_x}
    place_y = {1: up_y, 0: me_y, -1: down_y}

    def device(dx, dy):
        return {gx: place_x[dx], gy: place_y[dy]}

    pairs = (rows - 2) // 2
    edge_y = (cols - 1, 0)

    def load(start, count, sem):
        planes = pl.ds(start, count)
        return pltpu.make_async_copy(
            f_hbm.at[:, planes], field.at[:, planes, pl.ds(0, cols)], in_sem.at[sem]
        )

    barrier = pltpu.get_barrier_semaphore()
    around = [(dx, dy) for dx in (-1, 0, 1) for dy in (-1, 0, 1) if (dx, dy) != (0, 0)]
    for dx, dy in around:
        pl.semaphore_signal(barrier, inc=1, device_id=device(dx, dy), device_id_type=MESH)

    row_loads = []
    for side, y in enumerate(edge_y):
        row_loads.append(pltpu.make_async_copy(f_hbm.at[:, :, y], f_row.at[side], in_sem.at[0]))
        row_loads.append(pltpu.make_async_copy(solid_hbm.at[:, y], s_row.at[side], in_sem.at[1 + side]))
    load_solid = pltpu.make_async_copy(solid_hbm, solid, in_sem.at[3])
    ends = [load(0, 1, 4), load(rows - 1, 1, 4)]
    inner = [load(1 + 2 * c, 2, 5) for c in range(pairs)]
    for copy in row_loads + [load_solid] + ends + inner:
        copy.start()

    def wait_rows():
        both = (slice(None), pl.ds(0, 2), pl.ds(0, rows))
        pltpu.make_async_copy(f_hbm.at[both], field.at[both], in_sem.at[0]).wait()
        row_loads[1].wait()
        row_loads[3].wait()

    def remote(src, dst, phase, dx, dy):
        return pltpu.make_async_remote_copy(
            src_ref=src,
            dst_ref=dst,
            send_sem=send_sem.at[0],
            recv_sem=recv_sem.at[phase],
            device_id=device(dx, dy),
            device_id_type=MESH,
        )

    def x_copies(phase):
        buf = buffers[phase]
        own = pl.ds(PAD, cols)
        up, down = pl.ds(0, 5), pl.ds(8, 5)
        return [
            remote(buf.at[up, rows, own], buf.at[up, 0, own], phase, 1, 0),
            remote(buf.at[down, 1, own], buf.at[down, rows + 1, own], phase, -1, 0),
        ]

    def corner_copies(phase):
        buf = buffers[phase]
        copies = []
        for index in CORNERS:
            cx, cy, _ = VELOCITY[index]
            side = 0 if cy > 0 else 1
            j = (UP_Y, DOWN_Y)[side].index(index)
            src_x, dst_x = (rows - 1, 0) if cx > 0 else (0, rows + 1)
            dst = buf.at[SLOT[index], dst_x, PAD - 1] if cy > 0 else buf.at[SLOT[index], dst_x + 1, 0]
            copies.append(remote(y_send.at[phase, side, j, src_x], dst, phase, cx, cy))
        return copies

    def y_copies(phase):
        buf = buffers[phase]
        return [
            remote(y_send.at[phase, 0], buf.at[pl.ds(4, 5), pl.ds(1, rows), PAD - 1], phase, 0, 1),
            remote(y_send.at[phase, 1, pl.ds(0, 4)], buf.at[pl.ds(12, 4), pl.ds(2, rows), 0], phase, 0, -1),
            remote(y_send.at[phase, 1, 4], buf.at[0, pl.ds(2, rows), 0], phase, 0, -1),
        ]

    def arrive(phase):
        view = flat[phase].at[0, pl.ds(0, sent)]
        remote(view, view, phase, 1, 0).wait_recv()

    def row(phase, side, g):
        fluid = s_row[side, pl.ds(8 * g, 8), :] == 0
        if phase == 0:
            f = [f_row[side, i, pl.ds(8 * g, 8), :] for i in range(19)]
        else:
            view = flat[phase - 1]

            def strided(slot, cx, cy):
                start = (8 * g + 1 - cx) * pitch + PAD + edge_y[side] - cy
                return view[slot, pl.ds(start, 8, stride=pitch), :]

            f = pull(strided)
        wanted = (UP_Y, DOWN_Y)[side]
        post = collide(f, fluid, wanted)
        for j, index in enumerate(wanted):
            y_send[phase, side, j, pl.ds(8 * g, 8), :] = post[index]

    def advance(phase, x, t):
        fluid = solid[x, pl.ds(8 * t, 8), :] == 0
        if phase == 0:
            f = [field[i, x, pl.ds(8 * t, 8), :] for i in range(19)]
        else:
            f = pull(tile_load(buffers[phase - 1], x, t))
        post = collide(f, fluid)
        for i in range(19):
            buffers[phase][SLOT[i], x + 1, pl.ds(PAD + 8 * t, 8), :] = post[i]

    def plane(phase, x):
        for t in range(tiles):
            advance(phase, x, t)

    def start(copies):
        for copy in copies:
            copy.start()

    def edge_rows(phase):
        for side in range(2):
            for g in range(rows // 8):
                row(phase, side, g)

    def finish(x, t):
        f = pull(tile_load(p2, x, t))
        fluid = f[0] < BLOCKED
        for i in range(19):
            kept = field[i, x, pl.ds(8 * t, 8), :]
            field[i, x, pl.ds(8 * t, 8), :] = jnp.where(fluid, f[i], kept)

    odd = lax.rem(me_x, 2) == 1

    for phase in range(ITERS):
        if phase == 0:
            wait_rows()
        else:
            arrive(phase - 1)
        edge_rows(phase)
        x_up, x_down = x_copies(phase)
        if phase == 0:
            load_solid.wait()
            load(0, 2, 4).wait()
            plane(phase, rows - 1)
            plane(phase, 0)
            pl.semaphore_wait(barrier, len(around))
        start(corner_copies(phase))

        start(y_copies(phase))
        if phase:
            plane(phase, rows - 1)
        x_up.start()
        if phase:
            plane(phase, 0)
        x_down.start()
        if phase == 0:
            load(1, rows - 2, 5).wait()

        def step(x, carry):
            plane(phase, x)
            return carry

        lax.fori_loop(1, rows - 1, step, 0)

    def finish_step(c, carry):
        for dx in range(2):
            for t in range(1, tiles - 1):
                finish(1 + 2 * c + dx, t)
        return carry

    lax.fori_loop(0, pairs, finish_step, 0)

    view = flat[0].at[pl.ds(0, ITERS), pl.ds(0, sent)]
    remote(view, view, 0, 1, 0).wait_send()
    arrive(ITERS - 1)


def finish_kernel(buf, field, out, stage, sem):
    count, rows, cols, _ = out.shape
    tiles = cols // 8
    pairs = rows // 2
    inside = pl.ds(8, cols - 16)
    edges = (0, tiles - 1)

    def inner_copy(c):
        where = (slice(None), pl.ds(1 + 2 * c, 2), inside)
        return pltpu.make_async_copy(field.at[where], out.at[where], sem.at[0])

    def edge_copy(c, k):
        where = (slice(None), pl.ds(2 * c, 2), pl.ds(8 * edges[k], 8))
        return pltpu.make_async_copy(stage.at[where], out.at[where], sem.at[0])

    def end_copy(x, k):
        where = (slice(None), x, inside)
        return pltpu.make_async_copy(stage.at[where], out.at[where], sem.at[0])

    def finish(x, t):
        f = pull(tile_load(buf, x, t))
        fluid = f[0] < BLOCKED
        for i in range(count):
            kept = field[i, x, pl.ds(8 * t, 8), :]
            stage[i, x, pl.ds(8 * t, 8), :] = jnp.where(fluid, f[i], kept)

    for c in range(pairs - 1):
        inner_copy(c).start()
    for k, x in enumerate((0, rows - 1)):
        for t in range(1, tiles - 1):
            finish(x, t)
        end_copy(x, k).start()

    def step(c, carry):
        for dx in range(2):
            for t in edges:
                finish(2 * c + dx, t)
        for k in range(2):
            edge_copy(c, k).start()
        return carry

    lax.fori_loop(0, pairs, step, 0)
    pltpu.make_async_copy(stage.at[:, pl.ds(0, rows), pl.ds(0, cols)], out, sem.at[0]).wait()


def solution(mesh):
    gx, gy = mesh.axis_names
    gx_size, gy_size = mesh.shape[gx], mesh.shape[gy]

    def local(populations, solid):
        count, rows, cols, lanes = populations.shape
        f32 = jnp.float32
        padded = (count, rows + 3, cols + PAD, lanes)
        spaced = (count, rows + 1, cols + PAD, lanes)
        vmem = pl.BlockSpec(memory_space=pltpu.VMEM)
        hbm = pl.BlockSpec(memory_space=pltpu.HBM)
        post, field = pl.pallas_call(
            functools.partial(step_kernel, (rows, cols, gx_size, gy_size), (gx, gy)),
            out_shape=(
                jax.ShapeDtypeStruct(padded, f32),
                jax.ShapeDtypeStruct(spaced, f32),
            ),
            in_specs=[hbm, hbm],
            out_specs=(vmem, vmem),
            scratch_shapes=[
                pltpu.VMEM((rows, cols, lanes), jnp.int32),
                pltpu.VMEM(padded, f32),
                pltpu.VMEM(padded, f32),
                pltpu.VMEM((2, count, rows, lanes), f32),
                pltpu.VMEM((2, rows, lanes), jnp.int32),
                pltpu.VMEM((ITERS, 2, 5, rows, lanes), f32),
                pltpu.SemaphoreType.DMA((6,)),
                pltpu.SemaphoreType.DMA((1,)),
                pltpu.SemaphoreType.DMA((ITERS,)),
            ],
            compiler_params=pltpu.CompilerParams(
                collective_id=0, has_side_effects=True, vmem_limit_bytes=30 * 1024 * 1024
            ),
        )(
            pltpu.with_memory_space_constraint(populations, pltpu.HBM),
            pltpu.with_memory_space_constraint(solid, pltpu.HBM),
        )
        return pl.pallas_call(
            finish_kernel,
            out_shape=jax.ShapeDtypeStruct(populations.shape, f32),
            in_specs=[vmem, vmem],
            out_specs=hbm,
            scratch_shapes=[
                pltpu.VMEM(spaced, f32),
                pltpu.SemaphoreType.DMA((1,)),
            ],
            compiler_params=pltpu.CompilerParams(vmem_limit_bytes=12 * 1024 * 1024),
        )(post, field)

    return jax.shard_map(
        local,
        mesh=mesh,
        in_specs=(P(None, gx, gy, None), P(gx, gy, None)),
        out_specs=P(None, gx, gy, None),
        check_vma=False,
    )
```

```python
import functools

import jax
import jax.numpy as jnp
from jax import lax
from jax.experimental import pallas as pl
from jax.experimental.pallas import tpu as pltpu
from jax.sharding import PartitionSpec as P

ITERS = 3
MESH = pl.DeviceIdType.MESH

VELOCITY = (
    (0, 0, 0),
    (1, 0, 0), (-1, 0, 0), (0, 1, 0), (0, -1, 0), (0, 0, 1), (0, 0, -1),
    (1, 1, 0), (-1, -1, 0), (1, -1, 0), (-1, 1, 0),
    (1, 0, 1), (-1, 0, -1), (1, 0, -1), (-1, 0, 1),
    (0, 1, 1), (0, -1, -1), (0, 1, -1), (0, -1, 1),
)
RELAX = 1.6
BIG = 1e37
BLOCKED = 1e34

ORDER = [9, 1, 11, 13, 7, 3, 15, 17, 10, 2, 12, 14, 8, 4, 16, 18, 0, 5, 6]
SLOT = {index: slot for slot, index in enumerate(ORDER)}
UP_Y = [7, 3, 15, 17, 10]
DOWN_Y = [8, 4, 16, 18, 9]
CORNERS = (7, 8, 9, 10)
PAD = 8


def opposite(index):
    if index == 0:
        return 0
    return index + 1 if index % 2 == 1 else index - 1


def collide(f, fluid, wanted=range(19)):
    total = {}
    delta = {}
    for i in range(1, 19, 2):
        total[i] = f[i] + f[i + 1]
        delta[i] = f[i] - f[i + 1]
    rho = f[0] + ((total[1] + total[3]) + (total[5] + total[7])) + (
        ((total[9] + total[11]) + (total[13] + total[15])) + total[17]
    )
    mx = (delta[1] + delta[7]) + (delta[9] + delta[11]) + delta[13]
    my = (delta[3] + delta[7]) + (delta[15] - delta[9]) + delta[17]
    mz = (delta[5] + delta[11]) + (delta[15] - delta[13]) - delta[17]
    zero = jnp.zeros_like(rho)
    scale = RELAX * 3.0 / 36.0
    mx = jnp.where(fluid, mx * scale, zero)
    my = jnp.where(fluid, my * scale, zero)
    mz = jnp.where(fluid, mz * scale, zero)
    inv = 1.0 / rho
    curve = inv * (RELAX * 4.5 / 36.0 / (scale * scale))
    base = rho * (RELAX / 36.0) - (mx * mx + my * my + mz * mz) * (
        inv * (RELAX * 1.5 / 36.0 / (scale * scale))
    )
    base = jnp.where(fluid, base, jnp.full_like(rho, BIG * RELAX / 36.0))
    post = [None] * 19
    keep = 1.0 - RELAX
    half = keep * 0.5
    if 0 in wanted:
        post[0] = base * 12.0 + f[0] * keep
    base2 = base + base
    curve2 = curve + curve
    for i in range(1, 19, 2):
        if i not in wanted and i + 1 not in wanted:
            continue
        cx, cy, cz = VELOCITY[i]
        along = None
        for c, m in ((cx, mx), (cy, my), (cz, mz)):
            if c == 0:
                continue
            if along is None:
                along = m
            else:
                along = along + m if c > 0 else along - m
        if i < 7:
            even = base2 + along * along * curve2
            odd = along + along
        else:
            even = base + along * along * curve
            odd = along
        even = even + total[i] * half
        odd = odd + delta[i] * half
        if i in wanted:
            post[i] = even + odd
        if i + 1 in wanted:
            post[i + 1] = even - odd
    return post


def pull(load):
    own = [load(SLOT[i], 0, 0) for i in range(19)]
    f = [own[0]]
    for i in range(1, 19):
        cx, cy, cz = VELOCITY[i]
        value = own[i] if cx == 0 and cy == 0 else load(SLOT[i], cx, cy)
        if cz:
            value = pltpu.roll(value, 1 if cz > 0 else value.shape[1] - 1, axis=1)
        f.append(jnp.where(value > BLOCKED, own[opposite(i)], value))
    return f


def flatten(buf):
    count, planes, pitch, lanes = buf.shape
    return buf.reshape(count, planes * pitch, lanes)


def tile_load(buf, x, t):
    pitch = buf.shape[2]
    view = flatten(buf)

    def load(slot, cx, cy):
        first = PAD + 8 * t - cy
        if first + 8 > pitch:
            return view[slot, pl.ds((x + 1 - cx) * pitch + first, 8), :]
        return buf[slot, x + 1 - cx, pl.ds(first, 8), :]

    return load


def step_kernel(sizes, axes, f_hbm, solid_hbm, p2, field, solid, p0, p1, f_row, s_row, y_send, in_sem, send_sem, recv_sem):
    rows, cols, gx_size, gy_size = sizes
    gx, gy = axes
    tiles = cols // 8
    pitch = cols + PAD
    sent = 10 * (rows + cols) + len(CORNERS)
    buffers = (p0, p1, p2)
    flat = [flatten(buf) for buf in buffers]
    me_x, me_y = lax.axis_index(gx), lax.axis_index(gy)
    up_x, down_x = lax.rem(me_x + 1, gx_size), lax.rem(me_x + gx_size - 1, gx_size)
    up_y, down_y = lax.rem(me_y + 1, gy_size), lax.rem(me_y + gy_size - 1, gy_size)
    place_x = {1: up_x, 0: me_x, -1: down_x}
    place_y = {1: up_y, 0: me_y, -1: down_y}

    def device(dx, dy):
        return {gx: place_x[dx], gy: place_y[dy]}

    pairs = (rows - 2) // 2
    edge_y = (cols - 1, 0)

    def load(start, count, sem):
        planes = pl.ds(start, count)
        return pltpu.make_async_copy(
            f_hbm.at[:, planes], field.at[:, planes, pl.ds(0, cols)], in_sem.at[sem]
        )

    barrier = pltpu.get_barrier_semaphore()
    around = [(dx, dy) for dx in (-1, 0, 1) for dy in (-1, 0, 1) if (dx, dy) != (0, 0)]
    for dx, dy in around:
        pl.semaphore_signal(barrier, inc=1, device_id=device(dx, dy), device_id_type=MESH)

    row_loads = []
    for side, y in enumerate(edge_y):
        row_loads.append(pltpu.make_async_copy(f_hbm.at[:, :, y], f_row.at[side], in_sem.at[0]))
        row_loads.append(pltpu.make_async_copy(solid_hbm.at[:, y], s_row.at[side], in_sem.at[1 + side]))
    load_solid = pltpu.make_async_copy(solid_hbm, solid, in_sem.at[3])
    ends = [load(0, 1, 4), load(rows - 1, 1, 4)]
    inner = [load(1 + 2 * c, 2, 5) for c in range(pairs)]
    for copy in row_loads + [load_solid] + ends + inner:
        copy.start()

    def wait_rows():
        both = (slice(None), pl.ds(0, 2), pl.ds(0, rows))
        pltpu.make_async_copy(f_hbm.at[both], field.at[both], in_sem.at[0]).wait()
        row_loads[1].wait()
        row_loads[3].wait()

    def remote(src, dst, phase, dx, dy):
        return pltpu.make_async_remote_copy(
            src_ref=src,
            dst_ref=dst,
            send_sem=send_sem.at[0],
            recv_sem=recv_sem.at[phase],
            device_id=device(dx, dy),
            device_id_type=MESH,
        )

    def x_copies(phase):
        buf = buffers[phase]
        up, down = pl.ds(0, 5), pl.ds(8, 5)
        halves = [pl.ds(PAD + h * (cols // 2), cols // 2) for h in range(2)]
        return (
            [remote(buf.at[up, rows, own], buf.at[up, 0, own], phase, 1, 0) for own in halves],
            [remote(buf.at[down, 1, own], buf.at[down, rows + 1, own], phase, -1, 0) for own in halves],
        )

    def corner_copies(phase):
        buf = buffers[phase]
        copies = []
        for index in CORNERS:
            cx, cy, _ = VELOCITY[index]
            side = 0 if cy > 0 else 1
            j = (UP_Y, DOWN_Y)[side].index(index)
            src_x, dst_x = (rows - 1, 0) if cx > 0 else (0, rows + 1)
            dst = buf.at[SLOT[index], dst_x, PAD - 1] if cy > 0 else buf.at[SLOT[index], dst_x + 1, 0]
            copies.append(remote(y_send.at[phase, side, j, src_x], dst, phase, cx, cy))
        return copies

    def y_copies(phase):
        buf = buffers[phase]
        return [
            remote(y_send.at[phase, 0], buf.at[pl.ds(4, 5), pl.ds(1, rows), PAD - 1], phase, 0, 1),
            remote(y_send.at[phase, 1, pl.ds(0, 4)], buf.at[pl.ds(12, 4), pl.ds(2, rows), 0], phase, 0, -1),
            remote(y_send.at[phase, 1, 4], buf.at[0, pl.ds(2, rows), 0], phase, 0, -1),
        ]

    def arrive(phase):
        view = flat[phase].at[0, pl.ds(0, sent)]
        remote(view, view, phase, 1, 0).wait_recv()

    def row(phase, side, g):
        fluid = s_row[side, pl.ds(8 * g, 8), :] == 0
        if phase == 0:
            f = [f_row[side, i, pl.ds(8 * g, 8), :] for i in range(19)]
        else:
            view = flat[phase - 1]

            def strided(slot, cx, cy):
                start = (8 * g + 1 - cx) * pitch + PAD + edge_y[side] - cy
                return view[slot, pl.ds(start, 8, stride=pitch), :]

            f = pull(strided)
        wanted = (UP_Y, DOWN_Y)[side]
        post = collide(f, fluid, wanted)
        for j, index in enumerate(wanted):
            y_send[phase, side, j, pl.ds(8 * g, 8), :] = post[index]

    def advance(phase, x, t):
        fluid = solid[x, pl.ds(8 * t, 8), :] == 0
        if phase == 0:
            f = [field[i, x, pl.ds(8 * t, 8), :] for i in range(19)]
        else:
            f = pull(tile_load(buffers[phase - 1], x, t))
        post = collide(f, fluid)
        for i in range(19):
            buffers[phase][SLOT[i], x + 1, pl.ds(PAD + 8 * t, 8), :] = post[i]

    def plane(phase, x):
        for t in range(tiles):
            advance(phase, x, t)

    def start(copies):
        for copy in copies:
            copy.start()

    def edge_rows(phase):
        for side in range(2):
            for g in range(rows // 8):
                row(phase, side, g)

    def finish(x, t):
        f = pull(tile_load(p2, x, t))
        fluid = f[0] < BLOCKED
        for i in range(19):
            kept = field[i, x, pl.ds(8 * t, 8), :]
            field[i, x, pl.ds(8 * t, 8), :] = jnp.where(fluid, f[i], kept)


    for phase in range(ITERS):
        if phase == 0:
            wait_rows()
        else:
            arrive(phase - 1)
        edge_rows(phase)
        x_up, x_down = x_copies(phase)
        if phase == 0:
            load_solid.wait()
            load(0, 2, 4).wait()
            plane(phase, rows - 1)
            plane(phase, 0)
            pl.semaphore_wait(barrier, len(around))
        start(corner_copies(phase))

        start(y_copies(phase))
        for x, copies in ((rows - 1, x_up), (0, x_down)):
            for h, copy in enumerate(copies):
                if phase:
                    for t in range(h * tiles // 2, (h + 1) * tiles // 2):
                        advance(phase, x, t)
                copy.start()
        if phase == 0:
            load(1, rows - 2, 5).wait()

        def step(x, carry):
            plane(phase, x)
            return carry

        lax.fori_loop(1, rows - 1, step, 0)

    def finish_step(c, carry):
        for dx in range(2):
            for t in range(1, tiles - 1):
                finish(1 + 2 * c + dx, t)
        return carry

    lax.fori_loop(0, pairs, finish_step, 0)

    view = flat[0].at[pl.ds(0, ITERS), pl.ds(0, sent)]
    remote(view, view, 0, 1, 0).wait_send()
    arrive(ITERS - 1)


def finish_kernel(buf, field, out, stage, sem):
    count, rows, cols, _ = out.shape
    tiles = cols // 8
    pairs = rows // 2
    inside = pl.ds(8, cols - 16)
    edges = (0, tiles - 1)

    def inner_copy(c):
        where = (slice(None), pl.ds(1 + 2 * c, 2), inside)
        return pltpu.make_async_copy(field.at[where], out.at[where], sem.at[0])

    def edge_copy(c, k):
        where = (slice(None), pl.ds(2 * c, 2), pl.ds(8 * edges[k], 8))
        return pltpu.make_async_copy(stage.at[where], out.at[where], sem.at[0])

    def end_copy(x, k):
        where = (slice(None), x, inside)
        return pltpu.make_async_copy(stage.at[where], out.at[where], sem.at[0])

    def finish(x, t):
        f = pull(tile_load(buf, x, t))
        fluid = f[0] < BLOCKED
        for i in range(count):
            kept = field[i, x, pl.ds(8 * t, 8), :]
            stage[i, x, pl.ds(8 * t, 8), :] = jnp.where(fluid, f[i], kept)

    for c in range(pairs - 1):
        inner_copy(c).start()
    for k, x in enumerate((0, rows - 1)):
        for t in range(1, tiles - 1):
            finish(x, t)
        end_copy(x, k).start()

    def step(c, carry):
        for dx in range(2):
            for t in edges:
                finish(2 * c + dx, t)
        for k in range(2):
            edge_copy(c, k).start()
        return carry

    lax.fori_loop(0, pairs, step, 0)
    pltpu.make_async_copy(stage.at[:, pl.ds(0, rows), pl.ds(0, cols)], out, sem.at[0]).wait()


def solution(mesh):
    gx, gy = mesh.axis_names
    gx_size, gy_size = mesh.shape[gx], mesh.shape[gy]

    def local(populations, solid):
        count, rows, cols, lanes = populations.shape
        f32 = jnp.float32
        padded = (count, rows + 3, cols + PAD, lanes)
        spaced = (count, rows + 1, cols + PAD, lanes)
        vmem = pl.BlockSpec(memory_space=pltpu.VMEM)
        hbm = pl.BlockSpec(memory_space=pltpu.HBM)
        post, field = pl.pallas_call(
            functools.partial(step_kernel, (rows, cols, gx_size, gy_size), (gx, gy)),
            out_shape=(
                jax.ShapeDtypeStruct(padded, f32),
                jax.ShapeDtypeStruct(spaced, f32),
            ),
            in_specs=[hbm, hbm],
            out_specs=(vmem, vmem),
            scratch_shapes=[
                pltpu.VMEM((rows, cols, lanes), jnp.int32),
                pltpu.VMEM(padded, f32),
                pltpu.VMEM(padded, f32),
                pltpu.VMEM((2, count, rows, lanes), f32),
                pltpu.VMEM((2, rows, lanes), jnp.int32),
                pltpu.VMEM((ITERS, 2, 5, rows, lanes), f32),
                pltpu.SemaphoreType.DMA((6,)),
                pltpu.SemaphoreType.DMA((1,)),
                pltpu.SemaphoreType.DMA((ITERS,)),
            ],
            compiler_params=pltpu.CompilerParams(
                collective_id=0, has_side_effects=True, vmem_limit_bytes=30 * 1024 * 1024
            ),
        )(
            pltpu.with_memory_space_constraint(populations, pltpu.HBM),
            pltpu.with_memory_space_constraint(solid, pltpu.HBM),
        )
        return pl.pallas_call(
            finish_kernel,
            out_shape=jax.ShapeDtypeStruct(populations.shape, f32),
            in_specs=[vmem, vmem],
            out_specs=hbm,
            scratch_shapes=[
                pltpu.VMEM(spaced, f32),
                pltpu.SemaphoreType.DMA((1,)),
            ],
            compiler_params=pltpu.CompilerParams(vmem_limit_bytes=12 * 1024 * 1024),
        )(post, field)

    return jax.shard_map(
        local,
        mesh=mesh,
        in_specs=(P(None, gx, gy, None), P(gx, gy, None)),
        out_specs=P(None, gx, gy, None),
        check_vma=False,
    )
```

```python
import functools

import jax
import jax.numpy as jnp
from jax import lax
from jax.experimental import pallas as pl
from jax.experimental.pallas import tpu as pltpu
from jax.sharding import PartitionSpec as P

ITERS = 3
MESH = pl.DeviceIdType.MESH

VELOCITY = (
    (0, 0, 0),
    (1, 0, 0), (-1, 0, 0), (0, 1, 0), (0, -1, 0), (0, 0, 1), (0, 0, -1),
    (1, 1, 0), (-1, -1, 0), (1, -1, 0), (-1, 1, 0),
    (1, 0, 1), (-1, 0, -1), (1, 0, -1), (-1, 0, 1),
    (0, 1, 1), (0, -1, -1), (0, 1, -1), (0, -1, 1),
)
RELAX = 1.6
BIG = 1e37
BLOCKED = 1e34

ORDER = [9, 1, 11, 13, 7, 3, 15, 17, 10, 2, 12, 14, 8, 4, 16, 18, 0, 5, 6]
SLOT = {index: slot for slot, index in enumerate(ORDER)}
UP_Y = [7, 3, 15, 17, 10]
DOWN_Y = [8, 4, 16, 18, 9]
CORNERS = (7, 8, 9, 10)
PAD = 8


def opposite(index):
    if index == 0:
        return 0
    return index + 1 if index % 2 == 1 else index - 1


def collide(f, fluid, wanted=range(19)):
    total = {}
    delta = {}
    for i in range(1, 19, 2):
        total[i] = f[i] + f[i + 1]
        delta[i] = f[i] - f[i + 1]
    rho = f[0] + ((total[1] + total[3]) + (total[5] + total[7])) + (
        ((total[9] + total[11]) + (total[13] + total[15])) + total[17]
    )
    mx = (delta[1] + delta[7]) + (delta[9] + delta[11]) + delta[13]
    my = (delta[3] + delta[7]) + (delta[15] - delta[9]) + delta[17]
    mz = (delta[5] + delta[11]) + (delta[15] - delta[13]) - delta[17]
    zero = jnp.zeros_like(rho)
    scale = RELAX * 3.0 / 36.0
    mx = jnp.where(fluid, mx * scale, zero)
    my = jnp.where(fluid, my * scale, zero)
    mz = jnp.where(fluid, mz * scale, zero)
    inv = 1.0 / rho
    curve = inv * (RELAX * 4.5 / 36.0 / (scale * scale))
    base = rho * (RELAX / 36.0) - (mx * mx + my * my + mz * mz) * (
        inv * (RELAX * 1.5 / 36.0 / (scale * scale))
    )
    base = jnp.where(fluid, base, jnp.full_like(rho, BIG * RELAX / 36.0))
    post = [None] * 19
    keep = 1.0 - RELAX
    half = keep * 0.5
    if 0 in wanted:
        post[0] = base * 12.0 + f[0] * keep
    base2 = base + base
    curve2 = curve + curve
    for i in range(1, 19, 2):
        if i not in wanted and i + 1 not in wanted:
            continue
        cx, cy, cz = VELOCITY[i]
        along = None
        for c, m in ((cx, mx), (cy, my), (cz, mz)):
            if c == 0:
                continue
            if along is None:
                along = m
            else:
                along = along + m if c > 0 else along - m
        if i < 7:
            even = base2 + along * along * curve2
            odd = along + along
        else:
            even = base + along * along * curve
            odd = along
        even = even + total[i] * half
        odd = odd + delta[i] * half
        if i in wanted:
            post[i] = even + odd
        if i + 1 in wanted:
            post[i + 1] = even - odd
    return post


def pull(load):
    own = [load(SLOT[i], 0, 0) for i in range(19)]
    f = [own[0]]
    for i in range(1, 19):
        cx, cy, cz = VELOCITY[i]
        value = own[i] if cx == 0 and cy == 0 else load(SLOT[i], cx, cy)
        if cz:
            value = pltpu.roll(value, 1 if cz > 0 else value.shape[1] - 1, axis=1)
        f.append(jnp.where(value > BLOCKED, own[opposite(i)], value))
    return f


def flatten(buf):
    count, planes, pitch, lanes = buf.shape
    return buf.reshape(count, planes * pitch, lanes)


def tile_load(buf, x, t):
    pitch = buf.shape[2]
    view = flatten(buf)

    def load(slot, cx, cy):
        first = PAD + 8 * t - cy
        if first + 8 > pitch:
            return view[slot, pl.ds((x + 1 - cx) * pitch + first, 8), :]
        return buf[slot, x + 1 - cx, pl.ds(first, 8), :]

    return load


def step_kernel(sizes, axes, f_hbm, solid_hbm, p2, field, solid, p0, p1, f_row, s_row, y_send, in_sem, send_sem, recv_sem):
    rows, cols, gx_size, gy_size = sizes
    gx, gy = axes
    tiles = cols // 8
    pitch = cols + PAD
    sent = 10 * (rows + cols) + len(CORNERS)
    buffers = (p0, p1, p2)
    flat = [flatten(buf) for buf in buffers]
    me_x, me_y = lax.axis_index(gx), lax.axis_index(gy)
    up_x, down_x = lax.rem(me_x + 1, gx_size), lax.rem(me_x + gx_size - 1, gx_size)
    up_y, down_y = lax.rem(me_y + 1, gy_size), lax.rem(me_y + gy_size - 1, gy_size)
    place_x = {1: up_x, 0: me_x, -1: down_x}
    place_y = {1: up_y, 0: me_y, -1: down_y}

    def device(dx, dy):
        return {gx: place_x[dx], gy: place_y[dy]}

    pairs = (rows - 2) // 2
    edge_y = (cols - 1, 0)

    def load(start, count, sem):
        planes = pl.ds(start, count)
        return pltpu.make_async_copy(
            f_hbm.at[:, planes], field.at[:, planes, pl.ds(0, cols)], in_sem.at[sem]
        )

    barrier = pltpu.get_barrier_semaphore()
    around = [(dx, dy) for dx in (-1, 0, 1) for dy in (-1, 0, 1) if (dx, dy) != (0, 0)]
    for dx, dy in around:
        pl.semaphore_signal(barrier, inc=1, device_id=device(dx, dy), device_id_type=MESH)

    row_loads = []
    for side, y in enumerate(edge_y):
        row_loads.append(pltpu.make_async_copy(f_hbm.at[:, :, y], f_row.at[side], in_sem.at[0]))
        row_loads.append(pltpu.make_async_copy(solid_hbm.at[:, y], s_row.at[side], in_sem.at[1 + side]))
    load_solid = pltpu.make_async_copy(solid_hbm, solid, in_sem.at[3])
    ends = [load(0, 1, 4), load(rows - 1, 1, 4)]
    inner = [load(1 + 2 * c, 2, 5) for c in range(pairs)]
    for copy in row_loads + [load_solid] + ends + inner:
        copy.start()

    def wait_rows():
        both = (slice(None), pl.ds(0, 2), pl.ds(0, rows))
        pltpu.make_async_copy(f_hbm.at[both], field.at[both], in_sem.at[0]).wait()
        row_loads[1].wait()
        row_loads[3].wait()

    def remote(src, dst, phase, dx, dy, kind=0):
        return pltpu.make_async_remote_copy(
            src_ref=src,
            dst_ref=dst,
            send_sem=send_sem.at[0],
            recv_sem=recv_sem.at[phase, kind],
            device_id=device(dx, dy),
            device_id_type=MESH,
        )

    def x_copies(phase, spans):
        buf = buffers[phase]
        up, down = pl.ds(0, 5), pl.ds(8, 5)
        spans = [pl.ds(PAD + 8 * first, 8 * count) for first, count in spans]
        return (
            [remote(buf.at[up, rows, own], buf.at[up, 0, own], phase, 1, 0, 1) for own in spans],
            [remote(buf.at[down, 1, own], buf.at[down, rows + 1, own], phase, -1, 0, 1) for own in spans],
        )

    def corner_copies(phase):
        buf = buffers[phase]
        copies = []
        for index in CORNERS:
            cx, cy, _ = VELOCITY[index]
            side = 0 if cy > 0 else 1
            j = (UP_Y, DOWN_Y)[side].index(index)
            src_x, dst_x = (rows - 1, 0) if cx > 0 else (0, rows + 1)
            dst = buf.at[SLOT[index], dst_x, PAD - 1] if cy > 0 else buf.at[SLOT[index], dst_x + 1, 0]
            copies.append(remote(y_send.at[phase, side, j, src_x], dst, phase, cx, cy))
        return copies

    def y_copies(phase):
        buf = buffers[phase]
        return [
            remote(y_send.at[phase, 0], buf.at[pl.ds(4, 5), pl.ds(1, rows), PAD - 1], phase, 0, 1),
            remote(y_send.at[phase, 1, pl.ds(0, 4)], buf.at[pl.ds(12, 4), pl.ds(2, rows), 0], phase, 0, -1),
            remote(y_send.at[phase, 1, 4], buf.at[0, pl.ds(2, rows), 0], phase, 0, -1),
        ]

    def arrive(phase, kind):
        count = 10 * cols if kind else 10 * rows + len(CORNERS)
        view = flat[phase].at[0, pl.ds(0, count)]
        remote(view, view, phase, 1, 0, kind).wait_recv()

    def row(phase, side, g):
        fluid = s_row[side, pl.ds(8 * g, 8), :] == 0
        if phase == 0:
            f = [f_row[side, i, pl.ds(8 * g, 8), :] for i in range(19)]
        else:
            view = flat[phase - 1]

            def strided(slot, cx, cy):
                start = (8 * g + 1 - cx) * pitch + PAD + edge_y[side] - cy
                return view[slot, pl.ds(start, 8, stride=pitch), :]

            f = pull(strided)
        wanted = (UP_Y, DOWN_Y)[side]
        post = collide(f, fluid, wanted)
        for j, index in enumerate(wanted):
            y_send[phase, side, j, pl.ds(8 * g, 8), :] = post[index]

    def advance(phase, x, t):
        fluid = solid[x, pl.ds(8 * t, 8), :] == 0
        if phase == 0:
            f = [field[i, x, pl.ds(8 * t, 8), :] for i in range(19)]
        else:
            f = pull(tile_load(buffers[phase - 1], x, t))
        post = collide(f, fluid)
        for i in range(19):
            buffers[phase][SLOT[i], x + 1, pl.ds(PAD + 8 * t, 8), :] = post[i]

    def plane(phase, x):
        for t in range(tiles):
            advance(phase, x, t)

    def start(copies):
        for copy in copies:
            copy.start()

    def edge_rows(phase):
        for side in range(2):
            for g in range(rows // 8):
                row(phase, side, g)

    def finish(x, t):
        f = pull(tile_load(p2, x, t))
        fluid = f[0] < BLOCKED
        for i in range(19):
            kept = field[i, x, pl.ds(8 * t, 8), :]
            field[i, x, pl.ds(8 * t, 8), :] = jnp.where(fluid, f[i], kept)


    middle, outer, whole = ((1, tiles - 2),), ((0, 1), (tiles - 1, 1)), ((0, tiles),)

    for phase in range(ITERS):
        if phase == 0:
            wait_rows()
        else:
            arrive(phase - 1, 1)
            for x, copies in zip((rows - 1, 0), x_copies(phase, middle)):
                for t in range(1, tiles - 1):
                    advance(phase, x, t)
                start(copies)
            arrive(phase - 1, 0)
        edge_rows(phase)
        if phase == 0:
            load_solid.wait()
            load(0, 2, 4).wait()
            plane(phase, rows - 1)
            plane(phase, 0)
            pl.semaphore_wait(barrier, len(around))
        start(corner_copies(phase))

        start(y_copies(phase))
        for x, copies in zip((rows - 1, 0), x_copies(phase, outer if phase else whole)):
            if phase:
                for t in (0, tiles - 1):
                    advance(phase, x, t)
            start(copies)

        if phase == 0:
            load(1, rows - 2, 5).wait()

        def step(x, carry):
            plane(phase, x)
            return carry

        lax.fori_loop(1, rows - 1, step, 0)

    def finish_step(c, carry):
        for dx in range(2):
            for t in range(1, tiles - 1):
                finish(1 + 2 * c + dx, t)
        return carry

    lax.fori_loop(0, pairs, finish_step, 0)

    view = flat[0].at[pl.ds(0, ITERS), pl.ds(0, sent)]
    remote(view, view, 0, 1, 0).wait_send()
    arrive(ITERS - 1, 1)
    arrive(ITERS - 1, 0)


def finish_kernel(buf, field, out, stage, sem):
    count, rows, cols, _ = out.shape
    tiles = cols // 8
    pairs = rows // 2
    inside = pl.ds(8, cols - 16)
    edges = (0, tiles - 1)

    def inner_copy(c):
        where = (slice(None), pl.ds(1 + 2 * c, 2), inside)
        return pltpu.make_async_copy(field.at[where], out.at[where], sem.at[0])

    def edge_copy(c, k):
        where = (slice(None), pl.ds(2 * c, 2), pl.ds(8 * edges[k], 8))
        return pltpu.make_async_copy(stage.at[where], out.at[where], sem.at[0])

    def end_copy(x, k):
        where = (slice(None), x, inside)
        return pltpu.make_async_copy(stage.at[where], out.at[where], sem.at[0])

    def finish(x, t):
        f = pull(tile_load(buf, x, t))
        fluid = f[0] < BLOCKED
        for i in range(count):
            kept = field[i, x, pl.ds(8 * t, 8), :]
            stage[i, x, pl.ds(8 * t, 8), :] = jnp.where(fluid, f[i], kept)

    for c in range(pairs - 1):
        inner_copy(c).start()
    for k, x in enumerate((0, rows - 1)):
        for t in range(1, tiles - 1):
            finish(x, t)
        end_copy(x, k).start()

    def step(c, carry):
        for dx in range(2):
            for t in edges:
                finish(2 * c + dx, t)
        for k in range(2):
            edge_copy(c, k).start()
        return carry

    lax.fori_loop(0, pairs, step, 0)
    pltpu.make_async_copy(stage.at[:, pl.ds(0, rows), pl.ds(0, cols)], out, sem.at[0]).wait()


def solution(mesh):
    gx, gy = mesh.axis_names
    gx_size, gy_size = mesh.shape[gx], mesh.shape[gy]

    def local(populations, solid):
        count, rows, cols, lanes = populations.shape
        f32 = jnp.float32
        padded = (count, rows + 3, cols + PAD, lanes)
        spaced = (count, rows + 1, cols + PAD, lanes)
        vmem = pl.BlockSpec(memory_space=pltpu.VMEM)
        hbm = pl.BlockSpec(memory_space=pltpu.HBM)
        post, field = pl.pallas_call(
            functools.partial(step_kernel, (rows, cols, gx_size, gy_size), (gx, gy)),
            out_shape=(
                jax.ShapeDtypeStruct(padded, f32),
                jax.ShapeDtypeStruct(spaced, f32),
            ),
            in_specs=[hbm, hbm],
            out_specs=(vmem, vmem),
            scratch_shapes=[
                pltpu.VMEM((rows, cols, lanes), jnp.int32),
                pltpu.VMEM(padded, f32),
                pltpu.VMEM(padded, f32),
                pltpu.VMEM((2, count, rows, lanes), f32),
                pltpu.VMEM((2, rows, lanes), jnp.int32),
                pltpu.VMEM((ITERS, 2, 5, rows, lanes), f32),
                pltpu.SemaphoreType.DMA((6,)),
                pltpu.SemaphoreType.DMA((1,)),
                pltpu.SemaphoreType.DMA((ITERS, 2)),
            ],
            compiler_params=pltpu.CompilerParams(
                collective_id=0, has_side_effects=True, vmem_limit_bytes=30 * 1024 * 1024
            ),
        )(
            pltpu.with_memory_space_constraint(populations, pltpu.HBM),
            pltpu.with_memory_space_constraint(solid, pltpu.HBM),
        )
        return pl.pallas_call(
            finish_kernel,
            out_shape=jax.ShapeDtypeStruct(populations.shape, f32),
            in_specs=[vmem, vmem],
            out_specs=hbm,
            scratch_shapes=[
                pltpu.VMEM(spaced, f32),
                pltpu.SemaphoreType.DMA((1,)),
            ],
            compiler_params=pltpu.CompilerParams(vmem_limit_bytes=12 * 1024 * 1024),
        )(post, field)

    return jax.shard_map(
        local,
        mesh=mesh,
        in_specs=(P(None, gx, gy, None), P(gx, gy, None)),
        out_specs=P(None, gx, gy, None),
        check_vma=False,
    )
```
